256 devices in a mesh: seq: 64 (over y, z_lo, x), tp: 4 (over z_hi, core).
Axes of the slice: x: 4, y: 4, z: 8 (z_hi: 2, z_lo: 4; z = z_hi * 4 + z_lo), core: 2. Of those that a mesh axis runs over, the one named last changes fastest.
Arguments:
- hidden_in: bfloat16 [16384, 4096], P('seq', 'tp'), may hold values from -6 to 6
- order: int32 [16384], P('seq'), may hold values from 0 to 16383, as said below
- segment: int32 [16384], replicated, may hold values from 0 to 31, never falling along the last dimension, each value on 1 to 2048 neighbouring positions
- norm_gain: float32 [4096], replicated, may hold values from 0.1 to 1.9
- w_query: bfloat16 [4096, 2048], P('seq', 'tp')
- w_key: bfloat16 [4096, 512], P('seq', 'tp'), may hold values from -0.09375 to 0.09375
- w_value: bfloat16 [4096, 512], P('seq', 'tp'), may hold values from -0.09375 to 0.09375
- w_out: bfloat16 [2048, 4096], P('seq', 'tp'), may hold values from -0.5 to 0.5
Outputs:
- attn_out: bfloat16 [16384, 4096], P('seq', 'tp')
The draws below stay inside these ranges and needn't reach their ends.
Inputs may be any that keep to these rules, and one draw needn't show every extreme that they name: order holds every position once; it is made of runs of 64 consecutive positions, each starting at a multiple of 64 and stored in rows that start at a multiple of 64. `segment`: never falls along positions.
All inputs are finite; a program needn't handle non-finite values.
Results may differ from the reference program's by a relative error of at most 0.014.
The reference program's roundings to bfloat16 on the way (of `normed`, `weights` and `attention`) count: a program that leaves them out, or rounds other values in their place, can miss the bound.
Values may be sent and summed in bfloat16 or wider, within the bound.
No kernel may reach another device: no remote copies, remote signals or barrier semaphores. Data moves between devices by JAX's collectives and lax.ppermute only.
A program may use at most 128 MiB of HBM per device.

```python
import math
import jax
import jax.numpy as jnp
import numpy as np
from jax import lax

D = 4096
HEADS = 16
KV_HEADS = 4
HD = 128
BLK = 64
TOKENS = 16384


def draw_order(key, part):
    blocks = TOKENS // BLK
    shuffled = jax.random.permutation(key, blocks).astype(jnp.int32)
    inside = jnp.arange(BLK, dtype=jnp.int32)
    return (shuffled[:, None] * BLK + inside[None, :]).reshape(-1).astype(jnp.int32)


def draw_w_query(key, part):
    base = jax.random.normal(key, (D, HEADS * HD), jnp.float32) * D ** (-0.5)
    return base.astype(jnp.bfloat16)


def level_of(rng, extent, pieces, low, high):
    factor_of, own = 1.0, jax.random.fold_in(rng, 6)
    for dim, blocks in pieces:
        heights = jnp.exp(jax.random.uniform(jax.random.fold_in(own, dim), (blocks,), jnp.float32, low / len(pieces), high / len(pieces)))
        factor_of = factor_of * jnp.repeat(heights, extent[dim] // blocks).reshape([-1 if axis == dim else 1 for axis in range(len(extent))])
    return factor_of


def length_profile(amount, total, bound, slope):
    portions = [(1 << 20) // math.isqrt(rank ** slope) + 1 for rank in range(2, amount + 1)]
    surplus, counts = total - bound - (amount - 1), [1] * (amount - 1)
    while surplus > 0:
        movable = [i for i in range(amount - 1) if counts[i] < bound]
        pool, left = sum([portions[i] for i in movable]), surplus
        for i in movable:
            addition = min(bound - counts[i], max(1, left * portions[i] // pool), surplus)
            counts[i] = counts[i] + addition
            surplus = surplus - addition
    return np.array([bound] + counts)


def uneven(rng, number_of, total, reach, lean):
    if number_of == 2:
        one = jax.random.randint(rng, (), max(1, total - reach), min(reach, total - 1) + 1)
        return jnp.stack([one, total - one])
    sizes = jnp.asarray(length_profile(number_of, total, reach, lean), jnp.int32)
    twos = (number_of - 1) // 2
    source_of, sink = sizes[1:1 + 2 * twos:2], sizes[2:2 + 2 * twos:2]
    room = jnp.minimum(source_of - 1, reach - sink)
    passed = jax.random.randint(jax.random.fold_in(rng, 1), (twos,), 0, 1 << 20) % (room + 1)
    sizes = sizes.at[1:1 + 2 * twos:2].set(source_of - passed).at[2:2 + 2 * twos:2].set(sink + passed)
    return sizes[jax.random.permutation(jax.random.fold_in(rng, 2), number_of)]


def gaussian(own_key, extent, scale, most, shards=(), kind=jnp.bfloat16):
    result = jax.random.normal(own_key, extent, jnp.float32) * scale
    if len(shards) > 0:
        result = level_of(own_key, extent, shards, -0.22, 0.18) * result
    return jnp.clip(result, min=-most, max=most).astype(kind)


def setup_inputs(seed: int = 0) -> dict:
    arg_keys = jax.random.split(jax.random.key(seed), 9)
    return {
        "hidden_in": gaussian(arg_keys[0], (TOKENS, D), 1.0, 6.0, ((0, 64), (1, 4))),
        "order": draw_order(jax.random.fold_in(arg_keys[8], 71), 0),
        "segment": jnp.searchsorted(jnp.cumsum(uneven(arg_keys[2], max(2, TOKENS // (8 * BLK)), TOKENS, min(32 * BLK, TOKENS // 2), 1)), jnp.arange(TOKENS), side="right").astype(jnp.int32),
        "norm_gain": jnp.clip(1.0 + 0.18 * jax.random.normal(arg_keys[3], (D,), jnp.float32), 0.1, 1.9),
        "w_query": draw_w_query(jax.random.fold_in(arg_keys[8], 71), 0),
        "w_key": gaussian(arg_keys[5], (D, KV_HEADS * HD), D ** -0.5, 0.09375, ((0, 64), (1, 4))),
        "w_value": gaussian(arg_keys[6], (D, KV_HEADS * HD), D ** -0.5, 0.09375, ((0, 64), (1, 4))),
        "w_out": gaussian(arg_keys[7], (HEADS * HD, D), (HEADS * HD // 16) ** -0.5, 0.5, ((0, 64), (1, 4))),
    }


THETA = 500000.0
EPS = 1e-05

def rotary(block, positions):
    head_dim = block.shape[-1]
    width = head_dim // 2
    frequency = THETA ** (-jnp.arange(width, dtype=jnp.float32) * 2.0 / head_dim)
    angle = positions.astype(jnp.float32)[:, None] * frequency[None, :]
    cosine = jnp.cos(angle)[:, None, :]
    sine = jnp.sin(angle)[:, None, :]
    first = block[..., :width]
    second = block[..., width:]
    return jnp.concatenate([first * cosine - second * sine, second * cosine + first * sine], axis=-1)

def reference(hidden_in, order, segment, norm_gain, w_query, w_key, w_value, w_out):
    wide = hidden_in.astype(jnp.float32)
    mean_square = lax.optimization_barrier(jnp.mean(wide * wide, axis=1, keepdims=True))
    normed = (wide * lax.rsqrt(mean_square + EPS) * norm_gain[None, :]).astype(jnp.bfloat16)
    query = jnp.dot(normed, w_query, preferred_element_type=jnp.float32).reshape(TOKENS, HEADS, HD)
    key = jnp.dot(normed, w_key, preferred_element_type=jnp.float32).reshape(TOKENS, KV_HEADS, HD)
    value = jnp.dot(normed, w_value, preferred_element_type=jnp.float32).reshape(TOKENS, KV_HEADS, HD)
    query = lax.optimization_barrier((rotary(query, order) * HD ** (-0.5)).astype(jnp.bfloat16))
    key = lax.optimization_barrier(rotary(key, order).astype(jnp.bfloat16))
    value = lax.optimization_barrier(value.astype(jnp.bfloat16))
    group = HEADS // KV_HEADS
    query_wide = query.astype(jnp.float32).reshape(TOKENS, KV_HEADS, group, HD)
    key_wide = key.astype(jnp.float32)
    value_wide = value.astype(jnp.float32)
    document = jnp.take(segment, order, axis=0)
    block_rows = min(256, TOKENS)

    def attend(index):
        start = (index * block_rows).astype(jnp.int32)
        rows_query = lax.dynamic_slice_in_dim(query_wide, start, block_rows, 0)
        rows_order = lax.dynamic_slice_in_dim(order, start, block_rows, 0)
        rows_document = lax.dynamic_slice_in_dim(document, start, block_rows, 0)
        scores = jnp.einsum('rkgd,ckd->rkgc', rows_query, key_wide)
        allowed = (order[None, :] <= rows_order[:, None]) & (document[None, :] == rows_document[:, None])
        scores = jnp.where(allowed[:, None, None, :], scores, -jnp.inf)
        top = lax.optimization_barrier(jnp.max(scores, axis=-1, keepdims=True))
        weights = jnp.exp(scores - top)
        total = lax.optimization_barrier(jnp.sum(weights, axis=-1))
        rounded = lax.optimization_barrier(weights.astype(jnp.bfloat16)).astype(jnp.float32)
        mixed = jnp.einsum('rkgc,ckd->rkgd', rounded, value_wide)
        return (mixed / total[..., None]).astype(jnp.bfloat16)
    blocks = lax.map(attend, jnp.arange(TOKENS // block_rows, dtype=jnp.int32))
    attention = blocks.reshape(TOKENS, HEADS * HD)
    return jnp.dot(attention, w_out, preferred_element_type=jnp.float32).astype(jnp.bfloat16)
```

```python
import jax
import jax.numpy as jnp
from jax import lax
from jax.experimental import pallas as pl
from jax.experimental.pallas import tpu as pltpu
from jax.sharding import Mesh
from jax.sharding import PartitionSpec as P

HD = 128
BLK = 64
SIDE = 4
ROWS = 4 * BLK
MARK = 16
SEQ = ("y", "zl", "x")
TP = ("zh", "c")
THETA = 500000.0
EPS = 1e-05
LOWEST = -1e30


def from_ahead(v, axis, k):
    return lax.ppermute(v, axis, [(i, (i - k) % SIDE) for i in range(SIDE)])


def swapped(v, axis):
    return lax.ppermute(v, axis, [(0, 1), (1, 0)])


def line_gather(v, axis):
    return [v] + [from_ahead(v, axis, k) for k in (1, 2, 3)]


def halves(pieces):
    return [jnp.concatenate(pieces[k : k + 2], axis=0) for k in (0, 2)]


def far_ring(low, high, axis):
    ahead_low = from_ahead(low, axis, 1)
    behind_high = from_ahead(high, axis, 3)
    ahead_high = from_ahead(high, axis, 1)
    behind_low = from_ahead(low, axis, 3)
    far_low = from_ahead(ahead_low, axis, 1)
    far_high = from_ahead(behind_high, axis, 3)
    return [low, high, ahead_low, ahead_high, far_low, far_high, behind_low, behind_high]


def place_blocks(refs, start, me, last_is_x):
    my, mz, mx = me
    for d in range(SIDE):
        for part in range(2):

            def step(i, carry, d=d, part=part):
                e, dz = 2 * part + i // SIDE, i % SIDE
                dx, dy = (d, e) if last_is_x else (e, d)
                s = ((my + dy) % SIDE) * 16 + ((mz + dz) % SIDE) * 4 + (mx + dx) % SIDE
                start(refs[2 * d + part].at[i], s)
                return carry

            lax.fori_loop(0, 8, step, 0)


def start_into(dst, sem, rows, cols=slice(None), taken=slice(None)):
    def start(src, s):
        at = pl.multiple_of(s * rows, rows)
        pltpu.make_async_copy(src.at[:, taken], dst.at[pl.ds(at, rows), cols], sem).start()

    return start


def wait_all(dst, sem):
    pltpu.make_async_copy(dst, dst, sem).wait()


def rotated(v, cos, sin):
    return v * cos + pltpu.roll(v, HD // 2, 1) * sin


def kv_kernel(me, ids, h0, h1, h2, h3, gain, cos, sin, *rest):
    normed, both, weights, sem = rest[16:]
    spot = me[0], me[1], me[2]
    ahead = pl.ds(0, HD)
    place_blocks(rest[:8], start_into(weights, sem, 64, pl.ds(0, HD), ahead), spot, True)
    place_blocks(rest[8:16], start_into(weights, sem, 64, pl.ds(HD, HD), ahead), spot, False)
    parts = (h0, h1, h2, h3)
    width = h0.shape[1]
    total = jnp.zeros((h0.shape[0], 1), jnp.float32)
    for h in parts:
        w = h[...].astype(jnp.float32)
        total = total + jnp.sum(w * w, axis=1, keepdims=True)
    scale = lax.rsqrt(total / (4 * width) + EPS)
    for k, h in enumerate(parts):
        w = h[...].astype(jnp.float32)
        g = gain[pl.ds(me[3] ^ k, 1), :]
        normed[k] = (w * scale * g).astype(jnp.bfloat16)
    row = lax.broadcasted_iota(jnp.int32, (MARK, HD), 0)
    block = row * HD + lax.broadcasted_iota(jnp.int32, (MARK, HD), 1)
    mark = jnp.zeros((MARK, HD), jnp.float32)
    for j in range(4):
        mark = jnp.where(block == ids[j], j + 1.0, mark)
    both[2 * ROWS :, :] = mark.astype(jnp.bfloat16)
    wait_all(weights, sem)
    acc = jnp.zeros((h0.shape[0], 2 * HD), jnp.float32)
    for k in range(4):
        at = pl.multiple_of((me[3] ^ k) * width, width)
        acc = acc + jnp.dot(normed[k], weights[pl.ds(at, width), :], preferred_element_type=jnp.float32)
    both[:ROWS, :] = rotated(acc[:, :HD], cos[...], sin[...]).astype(jnp.bfloat16)
    both[ROWS : 2 * ROWS, :] = acc[:, HD:].astype(jnp.bfloat16)


def q_kernel(me, normed, cos, sin, *rest):
    query, weights, sem = rest[16:]
    spot = me[0], me[1], me[2]
    half = query.shape[1] // 2
    taken = pl.ds(HD, half)
    place_blocks(rest[:8], start_into(weights, sem, 64, pl.ds(0, half), taken), spot, True)
    place_blocks(rest[8:16], start_into(weights, sem, 64, pl.ds(half, half), taken), spot, False)
    wait_all(weights, sem)
    width = normed.shape[2]
    acc = jnp.zeros(query.shape, jnp.float32)
    for k in range(4):
        at = pl.multiple_of((me[3] ^ k) * width, width)
        acc = acc + jnp.dot(normed[k], weights[pl.ds(at, width), :], preferred_element_type=jnp.float32)
    for h in range(query.shape[1] // HD):
        cols = slice(h * HD, (h + 1) * HD)
        query[:, cols] = (rotated(acc[:, cols], cos[...], sin[...]) * HD ** (-0.5)).astype(jnp.bfloat16)


def attention_kernel(me, low, high, query, starts, *rest):
    ks, vs = rest[:8], rest[8:16]
    mixed, key, value, table, where, sem_k, sem_v, sem_w = rest[16:]
    spot = me[0], me[1], me[2]
    place_blocks(vs, start_into(value, sem_v, ROWS + MARK), spot, False)
    place_blocks(ks, start_into(key, sem_k, ROWS), spot, True)
    wait_all(value, sem_v)
    found = jnp.zeros((MARK, HD), jnp.int32)
    for s in range(64):
        mark = value[s * (ROWS + MARK) + ROWS : (s + 1) * (ROWS + MARK), :].astype(jnp.int32)
        found = found + jnp.where(mark > 0, mark + (4 * s - 1), 0)
    table[...] = found
    copy = pltpu.make_async_copy(table, where, sem_w)
    copy.start()
    wait_all(key, sem_k)
    copy.wait()
    heads = query.shape[1] // HD
    span = 4 * BLK
    for j in range(4):
        at = slice(j * BLK, (j + 1) * BLK)
        q = jnp.concatenate([query[at, h * HD:(h + 1) * HD] for h in range(heads)], axis=0)
        first = jnp.concatenate([starts[at, :]] * heads, axis=0)
        last_block, first_block = high[j], low[j]
        inside = lax.broadcasted_iota(jnp.int32, (heads * BLK, 1), 0) % BLK
        position = last_block * BLK + inside
        lane = lax.broadcasted_iota(jnp.int32, (1, span), 1)

        def step(i, carry):
            top, total, acc = carry
            base = last_block - 4 * i - 3
            wanted = [jnp.maximum(base + n, 0) for n in range(4)]
            blocks = [where[w // HD, w % HD] for w in wanted]
            at_key = [pl.multiple_of(b * BLK, BLK) for b in blocks]
            at_value = [pl.multiple_of(b * BLK + (b // 4) * MARK, MARK) for b in blocks]
            k = jnp.concatenate([key[pl.ds(a, BLK), :] for a in at_key], axis=0)
            v = jnp.concatenate([value[pl.ds(a, BLK), :] for a in at_value], axis=0)
            s = lax.dot_general(q, k, (((1,), (1,)), ((), ())), preferred_element_type=jnp.float32)
            spots = base * BLK + lane
            s = jnp.where((spots >= first) & (spots <= position), s, LOWEST)
            new_top = jnp.maximum(top, jnp.max(s, axis=1, keepdims=True))
            w = jnp.exp(s - new_top)
            shrink = jnp.exp(top - new_top)
            total = total * shrink + jnp.sum(w, axis=1, keepdims=True)
            acc = acc * shrink + jnp.dot(w.astype(jnp.bfloat16), v, preferred_element_type=jnp.float32)
            return new_top, total, acc

        initial = (
            jnp.full((heads * BLK, 1), LOWEST, jnp.float32),
            jnp.zeros((heads * BLK, 1), jnp.float32),
            jnp.zeros((heads * BLK, HD), jnp.float32),
        )
        count = (last_block - first_block) // 4 + 1
        _, total, acc = lax.fori_loop(0, count, step, initial)
        result = (acc / total).astype(jnp.bfloat16)
        for h in range(heads):
            mixed[at, h * HD:(h + 1) * HD] = result[h * BLK:(h + 1) * BLK]


def near_out_kernel(me, m0, m1, *rest):
    partial, others, weights, sem = rest[16:]
    half, wide = others.shape[0], others.shape[1] // 2
    spot = me[0], me[1], me[2]
    place_blocks(rest[:8], start_into(weights, sem, 32, pl.ds(0, wide)), spot, True)
    place_blocks(rest[8:16], start_into(weights, sem, 32, pl.ds(wide, wide)), spot, False)
    wait_all(weights, sem)
    width = m0.shape[1]
    acc = jnp.zeros(partial.shape, jnp.float32)
    for k, m in enumerate((m0, m1)):
        at = pl.multiple_of((me[3] ^ k) * width, width)
        acc = acc + jnp.dot(m[...], weights[pl.ds(at, width), :], preferred_element_type=jnp.float32)
    partial[...] = acc
    far = pl.multiple_of((1 - me[3] // 2) * half, half)
    others[...] = weights[pl.ds(far, half), :]


def far_out_kernel(me, m2, m3, partial, others, out):
    width = m2.shape[1]
    acc = partial[...]
    for k, m in enumerate((m2, m3)):
        at = pl.multiple_of((me[3] % 2 ^ k) * width, width)
        acc = acc + jnp.dot(m[...], others[pl.ds(at, width), :], preferred_element_type=jnp.float32)
    out[...] = acc.astype(jnp.bfloat16)


SM = pl.BlockSpec(memory_space=pltpu.SMEM)
VM = pl.BlockSpec(memory_space=pltpu.VMEM)
HB = pl.BlockSpec(memory_space=pl.ANY)


def call(body, out, specs, scratch, *args):
    many = isinstance(out, (list, tuple))
    return pl.pallas_call(
        body,
        out_shape=out,
        in_specs=specs,
        out_specs=[VM] * len(out) if many else VM,
        scratch_shapes=scratch,
        compiler_params=pltpu.CompilerParams(vmem_limit_bytes=48 << 20),
    )(*args)


def pack_kernel(p0, p1, p2, p3, first, second):
    cut = first.shape[1]
    for k, p in enumerate((p0, p1, p2, p3)):
        first[k] = p[:cut, :]
        second[k] = p[cut:, :]


def packed(pieces, cut):
    rows, cols = pieces[0].shape
    shapes = [jax.ShapeDtypeStruct((SIDE, n, cols), jnp.bfloat16) for n in (cut, rows - cut)]
    return call(pack_kernel, shapes, [VM] * 4, [], *pieces)


def exchange(v):
    near = swapped(v, "c")
    across = swapped(v, "zh")
    return v, near, across, swapped(across, "c")


def stages(hidden_in, order, segment, norm_gain, w_query, w_key, w_value, w_out):
    rows = hidden_in.shape[0]
    bf = jnp.bfloat16
    me = jnp.stack(
        [lax.axis_index("y"), lax.axis_index("zl"), lax.axis_index("x"), lax.axis_index("zh") * 2 + lax.axis_index("c")]
    ).astype(jnp.int32)

    ids = order[::BLK] // BLK
    document = jnp.take(segment, order, axis=0)
    starts = jnp.sum((segment[None, :] < document[:, None]).astype(jnp.int32), axis=1)
    low = starts[::BLK] // BLK
    half = HD // 2
    frequency = THETA ** (-jnp.arange(half, dtype=jnp.float32) * 2.0 / HD)
    angle = order.astype(jnp.float32)[:, None] * frequency[None, :]
    cosine, sine = jnp.cos(angle), jnp.sin(angle)
    cos = jnp.concatenate([cosine, cosine], axis=1)
    sin = jnp.concatenate([-sine, sine], axis=1)

    near = w_query.shape[1] // 2
    first = jnp.concatenate([w_key, w_query[:, :near]], axis=1)
    second = jnp.concatenate([w_value, w_query[:, near:]], axis=1)
    pieces = line_gather(jnp.concatenate([first, second], axis=0), "zl")
    lines_a, lines_b = packed(pieces, first.shape[0])
    hiddens = exchange(hidden_in)
    weights = far_ring(*halves(line_gather(lines_a, "y")), "x")
    weights += far_ring(*halves(line_gather(lines_b, "x")), "y")

    wide = w_out.shape[1] // 2
    tall = jnp.concatenate([w_out[:, :wide], w_out[:, wide:]], axis=0)
    lines_a, lines_b = packed(line_gather(tall, "zl"), w_out.shape[0])
    wo = far_ring(*halves(line_gather(lines_a, "y")), "x")
    wo += far_ring(*halves(line_gather(lines_b, "x")), "y")

    gain = norm_gain.reshape(4, -1)
    dma = pltpu.SemaphoreType.DMA
    normed, both = call(
        kv_kernel,
        [
            jax.ShapeDtypeStruct((4, rows, hidden_in.shape[1]), bf),
            jax.ShapeDtypeStruct((2 * ROWS + MARK, HD), bf),
        ],
        [SM] * 2 + [VM] * 7 + [HB] * 16,
        [pltpu.VMEM((4096, 2 * HD), bf), dma],
        me, ids, *hiddens, gain, cos, sin, *weights,
    )
    lines_k, lines_v = packed(line_gather(both, "zl"), ROWS)
    keys = far_ring(*halves(line_gather(lines_k, "y")), "x")
    values = far_ring(*halves(line_gather(lines_v, "x")), "y")
    query = call(
        q_kernel,
        jax.ShapeDtypeStruct((rows, w_query.shape[1]), bf),
        [SM] + [VM] * 3 + [HB] * 16,
        [pltpu.VMEM((4096, w_query.shape[1]), bf), dma],
        me, normed, cos, sin, *weights,
    )
    mixed = call(
        attention_kernel,
        jax.ShapeDtypeStruct(query.shape, bf),
        [SM] * 3 + [VM] * 2 + [HB] * 16,
        [
            pltpu.VMEM((64 * ROWS, HD), bf),
            pltpu.VMEM((64 * (ROWS + MARK), HD), bf),
            pltpu.VMEM((MARK, HD), jnp.int32),
            pltpu.SMEM((MARK, HD), jnp.int32),
            dma, dma, dma,
        ],
        me, low, ids, query, starts[:, None], *keys, *values,
    )
    m0, m1, m2, m3 = exchange(mixed)
    partial, others = call(
        near_out_kernel,
        [jax.ShapeDtypeStruct((rows, w_out.shape[1]), jnp.float32), jax.ShapeDtypeStruct((1024, w_out.shape[1]), bf)],
        [SM] + [VM] * 2 + [HB] * 16,
        [pltpu.VMEM((2048, w_out.shape[1]), bf), dma],
        me, m0, m1, *wo,
    )
    return call(
        far_out_kernel,
        jax.ShapeDtypeStruct((rows, w_out.shape[1]), bf),
        [SM] + [VM] * 4,
        [],
        me, m2, m3, partial, others,
    )


def solution(mesh):
    torus = Mesh(mesh.devices.reshape(4, 4, 4, 2, 2), SEQ + TP)
    placed = (P(SEQ, TP), P(SEQ), P(), P(), P(SEQ, TP), P(SEQ, TP), P(SEQ, TP), P(SEQ, TP))
    return jax.shard_map(stages, mesh=torus, in_specs=placed, out_specs=P(SEQ, TP), check_vma=False)
```

```python
import jax
import jax.numpy as jnp
from jax import lax
from jax.experimental import pallas as pl
from jax.experimental.pallas import tpu as pltpu
from jax.sharding import Mesh
from jax.sharding import PartitionSpec as P

HD = 128
BLK = 64
SIDE = 4
ROWS = 4 * BLK
MARK = 16
SPAN = 4
SEQ = ("y", "zl", "x")
TP = ("zh", "c")
THETA = 500000.0
EPS = 1e-05
LOWEST = -1e30


def from_ahead(v, axis, k):
    return lax.ppermute(v, axis, [(i, (i - k) % SIDE) for i in range(SIDE)])


def swapped(v, axis):
    return lax.ppermute(v, axis, [(0, 1), (1, 0)])


def line_gather(v, axis):
    return [v] + [from_ahead(v, axis, k) for k in (1, 2, 3)]


def halves(pieces):
    return [jnp.concatenate(pieces[k : k + 2], axis=0) for k in (0, 2)]


def near_ring(low, high, axis):
    both = jnp.concatenate([low, high], axis=0)
    return [both] + [from_ahead(both, axis, k) for k in (1, 2, 3)]


def far_ring(low, high, axis):
    ahead_low = from_ahead(low, axis, 1)
    behind_high = from_ahead(high, axis, 3)
    ahead_high = from_ahead(high, axis, 1)
    behind_low = from_ahead(low, axis, 3)
    far_low = from_ahead(ahead_low, axis, 1)
    far_high = from_ahead(behind_high, axis, 3)
    return [low, high, ahead_low, ahead_high, far_low, far_high, behind_low, behind_high]


def place_blocks(refs, dst, me, last_is_x, cols=slice(None)):
    my, mz, mx = me
    rows = refs[0].shape[1]
    per = len(refs) // SIDE
    for d in range(SIDE):
        for part in range(per):

            def step(i, carry, d=d, part=part):
                e, dz = SIDE // per * part + i // SIDE, i % SIDE
                dx, dy = (d, e) if last_is_x else (e, d)
                s = ((my + dy) % SIDE) * 16 + ((mz + dz) % SIDE) * 4 + (mx + dx) % SIDE
                dst[pl.ds(pl.multiple_of(s * rows, rows), rows), cols] = refs[per * d + part][i]
                return carry

            lax.fori_loop(0, 16 // per, step, 0, unroll=2)


def rotated(v, cos, sin):
    return v * cos + pltpu.roll(v, HD // 2, 1) * sin


def prep_kernel(order, segment, starts, low):
    lane = lax.broadcasted_iota(jnp.int32, (BLK, HD), 1)
    row = lax.broadcasted_iota(jnp.int32, (BLK, HD), 0)
    whole = segment[...].astype(jnp.float32)
    for j in range(4):
        block = order[j * BLK] // BLK
        line = segment[pl.ds(block // 2, 1), :].astype(jnp.float32)
        shift = (block % 2) * BLK
        inside = (lane >= shift) & (lane < shift + BLK)
        own = jnp.sum(jnp.where(lane == row + shift, line, 0.0), axis=1, keepdims=True)
        first = jnp.min(own)
        begin = jnp.sum(jnp.where(whole < first, 1.0, 0.0))
        before = jnp.sum(jnp.where(inside & (line < own), 1.0, 0.0), axis=1, keepdims=True)
        base = (block * BLK).astype(jnp.float32)
        starts[j * BLK : (j + 1) * BLK, :] = jnp.where(own == first, begin, base + before).astype(jnp.int32)
        low[j] = begin.astype(jnp.int32) // BLK


def qkv_kernel(me, order, h0, h1, h2, h3, gain, cos, sin, *rest):
    both, query, normed, weights = rest[16:]
    spot = me[0], me[1], me[2]
    side = weights.shape[1] // 2
    place_blocks(rest[:8], weights, spot, True, slice(0, side))
    place_blocks(rest[8:16], weights, spot, False, slice(side, 2 * side))
    parts = (h0, h1, h2, h3)
    width = h0.shape[1]
    total = jnp.zeros((h0.shape[0], 1), jnp.float32)
    for h in parts:
        w = h[...].astype(jnp.float32)
        total = total + jnp.sum(w * w, axis=1, keepdims=True)
    scale = lax.rsqrt(total / (4 * width) + EPS)
    for k, h in enumerate(parts):
        w = h[...].astype(jnp.float32)
        g = gain[pl.ds(me[3] ^ k, 1), :]
        normed[k] = (w * scale * g).astype(jnp.bfloat16)
    row = lax.broadcasted_iota(jnp.int32, (MARK, HD), 0)
    block = row * HD + lax.broadcasted_iota(jnp.int32, (MARK, HD), 1)
    mark = jnp.zeros((MARK, HD), jnp.float32)
    for j in range(4):
        mark = jnp.where(block == order[j * BLK] // BLK, j + 1.0, mark)
    both[2 * ROWS :, :] = mark.astype(jnp.bfloat16)
    for n in range(2):
        acc = jnp.zeros((h0.shape[0], side), jnp.float32)
        for k in range(4):
            at = pl.multiple_of((me[3] ^ k) * width, width)
            w = weights[pl.ds(at, width), n * side : (n + 1) * side]
            acc = acc + jnp.dot(normed[k], w, preferred_element_type=jnp.float32)
        own = acc[:, :HD] if n else rotated(acc[:, :HD], cos[...], sin[...])
        both[n * ROWS : (n + 1) * ROWS, :] = own.astype(jnp.bfloat16)
        for h in range(2):
            q = rotated(acc[:, (h + 1) * HD : (h + 2) * HD], cos[...], sin[...]) * HD ** (-0.5)
            query[:, (2 * n + h) * HD : (2 * n + h + 1) * HD] = q.astype(jnp.bfloat16)


def attention_kernel(me, low, order, query, starts, *rest):
    ks, vs = rest[:8], rest[8:16]
    mixed, key, value, table, where, sem = rest[16:]
    spot = me[0], me[1], me[2]
    place_blocks(vs, value, spot, False)
    found = jnp.zeros((MARK, HD), jnp.int32)
    for s in range(64):
        mark = value[s * (ROWS + MARK) + ROWS : (s + 1) * (ROWS + MARK), :].astype(jnp.int32)
        found = found + jnp.where(mark > 0, mark + (4 * s - 1), 0)
    table[...] = found
    copy = pltpu.make_async_copy(table, where, sem)
    copy.start()
    place_blocks(ks, key, spot, True)
    copy.wait()
    heads = query.shape[1] // HD
    span = SPAN * BLK
    for j in range(4):
        at = slice(j * BLK, (j + 1) * BLK)
        q = jnp.concatenate([query[at, h * HD:(h + 1) * HD] for h in range(heads)], axis=0)
        first = jnp.concatenate([starts[at, :]] * heads, axis=0)
        last_block, first_block = order[j * BLK] // BLK, low[j]
        inside = lax.broadcasted_iota(jnp.int32, (heads * BLK, 1), 0) % BLK
        position = last_block * BLK + inside
        lane = lax.broadcasted_iota(jnp.int32, (1, span), 1)

        def step(i, carry):
            top, total, acc = carry
            base = last_block - SPAN * i - (SPAN - 1)
            wanted = [jnp.maximum(base + n, 0) for n in range(SPAN)]
            blocks = [where[w // HD, w % HD] for w in wanted]
            at_key = [pl.multiple_of(b * BLK, BLK) for b in blocks]
            at_value = [pl.multiple_of(b * BLK + (b // 4) * MARK, MARK) for b in blocks]
            k = jnp.concatenate([key[pl.ds(a, BLK), :] for a in at_key], axis=0)
            v = jnp.concatenate([value[pl.ds(a, BLK), :] for a in at_value], axis=0)
            s = lax.dot_general(q, k, (((1,), (1,)), ((), ())), preferred_element_type=jnp.float32)
            spots = base * BLK + lane
            s = jnp.where((spots >= first) & (spots <= position), s, LOWEST)
            new_top = jnp.maximum(top, jnp.max(s, axis=1, keepdims=True))
            w = jnp.exp(s - new_top)
            shrink = jnp.exp(top - new_top)
            total = total * shrink + jnp.sum(w, axis=1, keepdims=True)
            acc = acc * shrink + jnp.dot(w.astype(jnp.bfloat16), v, preferred_element_type=jnp.float32)
            return new_top, total, acc

        initial = (
            jnp.full((heads * BLK, 1), LOWEST, jnp.float32),
            jnp.zeros((heads * BLK, 1), jnp.float32),
            jnp.zeros((heads * BLK, HD), jnp.float32),
        )
        count = (last_block - first_block) // SPAN + 1
        _, total, acc = lax.fori_loop(0, count, step, initial)
        result = (acc / total).astype(jnp.bfloat16)
        for h in range(heads):
            mixed[at, h * HD:(h + 1) * HD] = result[h * BLK:(h + 1) * BLK]


def near_out_kernel(me, m0, m1, *rest):
    partial, others, weights = rest[8:]
    half, wide = others.shape[0], others.shape[1] // 2
    spot = me[0], me[1], me[2]
    place_blocks(rest[:4], weights, spot, True, slice(0, wide))
    place_blocks(rest[4:8], weights, spot, False, slice(wide, 2 * wide))
    width = m0.shape[1]
    acc = jnp.zeros(partial.shape, jnp.float32)
    for k, m in enumerate((m0, m1)):
        at = pl.multiple_of((me[3] ^ k) * width, width)
        acc = acc + jnp.dot(m[...], weights[pl.ds(at, width), :], preferred_element_type=jnp.float32)
    partial[...] = acc
    far = pl.multiple_of((1 - me[3] // 2) * half, half)
    others[...] = weights[pl.ds(far, half), :]


def far_out_kernel(me, m2, m3, partial, others, out):
    width = m2.shape[1]
    acc = partial[...]
    for k, m in enumerate((m2, m3)):
        at = pl.multiple_of((me[3] % 2 ^ k) * width, width)
        acc = acc + jnp.dot(m[...], others[pl.ds(at, width), :], preferred_element_type=jnp.float32)
    out[...] = acc.astype(jnp.bfloat16)


SM = pl.BlockSpec(memory_space=pltpu.SMEM)
VM = pl.BlockSpec(memory_space=pltpu.VMEM)


def call(body, out, specs, scratch, *args, outs=None):
    many = isinstance(out, (list, tuple))
    return pl.pallas_call(
        body,
        out_shape=out,
        in_specs=specs,
        out_specs=outs or ([VM] * len(out) if many else VM),
        scratch_shapes=scratch,
        compiler_params=pltpu.CompilerParams(vmem_limit_bytes=24 << 20),
    )(*args)


def pack_kernel(p0, p1, p2, p3, first, second):
    cut = first.shape[1]
    for k, p in enumerate((p0, p1, p2, p3)):
        first[k] = p[:cut, :]
        second[k] = p[cut:, :]


def packed(pieces, cut):
    rows, cols = pieces[0].shape
    shapes = [jax.ShapeDtypeStruct((SIDE, n, cols), jnp.bfloat16) for n in (cut, rows - cut)]
    return call(pack_kernel, shapes, [VM] * 4, [], *pieces)


def exchange(v):
    near = swapped(v, "c")
    across = swapped(v, "zh")
    return v, near, across, swapped(across, "c")


def stages(hidden_in, order, segment, norm_gain, w_query, w_key, w_value, w_out):
    rows = hidden_in.shape[0]
    bf = jnp.bfloat16
    me = jnp.stack(
        [lax.axis_index("y"), lax.axis_index("zl"), lax.axis_index("x"), lax.axis_index("zh") * 2 + lax.axis_index("c")]
    ).astype(jnp.int32)

    starts, low = call(
        prep_kernel,
        [jax.ShapeDtypeStruct((rows, 1), jnp.int32), jax.ShapeDtypeStruct((4,), jnp.int32)],
        [SM, VM],
        [],
        order, segment.reshape(-1, HD),
        outs=[VM, SM],
    )
    half = HD // 2
    frequency = THETA ** (-jnp.arange(half, dtype=jnp.float32) * 2.0 / HD)
    angle = order.astype(jnp.float32)[:, None] * frequency[None, :]
    cosine, sine = jnp.cos(angle), jnp.sin(angle)
    cos = jnp.concatenate([cosine, cosine], axis=1)
    sin = jnp.concatenate([-sine, sine], axis=1)

    near = w_query.shape[1] // 2
    first = jnp.concatenate([w_key, w_query[:, :near]], axis=1)
    second = jnp.concatenate([w_value, w_query[:, near:]], axis=1)
    pieces = line_gather(jnp.concatenate([first, second], axis=0), "zl")
    wide = w_out.shape[1] // 2
    tall = jnp.concatenate([w_out[:, :wide], w_out[:, wide:]], axis=0)
    gain = norm_gain.reshape(4, -1)
    pieces, cos, sin, gain, tall, me = lax.optimization_barrier((pieces, cos, sin, gain, tall, me))
    lines_a, lines_b = packed(pieces, first.shape[0])
    hiddens = exchange(hidden_in)
    weights = far_ring(*halves(line_gather(lines_a, "y")), "x")
    weights += far_ring(*halves(line_gather(lines_b, "x")), "y")

    lines_a, lines_b = packed(line_gather(tall, "zl"), w_out.shape[0])
    wo = near_ring(*halves(line_gather(lines_a, "y")), "x")
    wo += near_ring(*halves(line_gather(lines_b, "x")), "y")

    both, query = call(
        qkv_kernel,
        [
            jax.ShapeDtypeStruct((2 * ROWS + MARK, HD), bf),
            jax.ShapeDtypeStruct((rows, w_query.shape[1]), bf),
        ],
        [SM] * 2 + [VM] * 23,
        [pltpu.VMEM((4, rows, hidden_in.shape[1]), bf), pltpu.VMEM((4096, 2 * first.shape[1]), bf)],
        me, order, *hiddens, gain, cos, sin, *weights,
    )
    lines_k, lines_v = packed(line_gather(both, "zl"), ROWS)
    keys = far_ring(*halves(line_gather(lines_k, "y")), "x")
    values = far_ring(*halves(line_gather(lines_v, "x")), "y")
    mixed = call(
        attention_kernel,
        jax.ShapeDtypeStruct(query.shape, bf),
        [SM] * 3 + [VM] * 18,
        [
            pltpu.VMEM((64 * ROWS, HD), bf),
            pltpu.VMEM((64 * (ROWS + MARK), HD), bf),
            pltpu.VMEM((MARK, HD), jnp.int32),
            pltpu.SMEM((MARK, HD), jnp.int32),
            pltpu.SemaphoreType.DMA,
        ],
        me, low, order, query, starts, *keys, *values,
    )
    m0, m1, m2, m3 = exchange(mixed)
    partial, others = call(
        near_out_kernel,
        [jax.ShapeDtypeStruct((rows, w_out.shape[1]), jnp.float32), jax.ShapeDtypeStruct((1024, w_out.shape[1]), bf)],
        [SM] + [VM] * 10,
        [pltpu.VMEM((2048, w_out.shape[1]), bf)],
        me, m0, m1, *wo,
    )
    return call(
        far_out_kernel,
        jax.ShapeDtypeStruct((rows, w_out.shape[1]), bf),
        [SM] + [VM] * 4,
        [],
        me, m2, m3, partial, others,
    )


def solution(mesh):
    torus = Mesh(mesh.devices.reshape(4, 4, 4, 2, 2), SEQ + TP)
    placed = (P(SEQ, TP), P(SEQ), P(), P(), P(SEQ, TP), P(SEQ, TP), P(SEQ, TP), P(SEQ, TP))
    return jax.shard_map(stages, mesh=torus, in_specs=placed, out_specs=P(SEQ, TP), check_vma=False)
```
